256 devices in a mesh: bank: 16 (over y, x), zero: 16 (over z, core).
Axes of the slice: x: 4, y: 4, z: 8, core: 2. Of those that a mesh axis runs over, the one named last changes fastest.
Arguments:
- w_down: float32 [64, 1024, 2048], P('bank', None, 'zero'), may hold values from -0.25 to 0.25
- avg_down: bfloat16 [64, 1024, 2048], P('bank', None, 'zero'), may hold values from -0.09375 to 0.09375
- router_weight: float32 [2048, 64], P('zero', 'bank'), may hold values from -0.125 to 0.125
- router_gain: float32 [2048], P('zero'), may hold values from 0.25 to 1.75
Outputs:
- serve_down: bfloat16 [64, 1024, 2048], P('bank')
- scale_down: float32 [64, 1024], P('bank')
- serve_router: bfloat16 [2048, 64], replicated
The draws below stay inside these ranges and needn't reach their ends.
All inputs are finite; a program needn't handle non-finite values.
Results may differ from the reference program's by a relative error of at most 0.001.
Values may be sent and summed in bfloat16 or wider, within the bound.
No kernel may reach another device: no remote copies, remote signals or barrier semaphores. Data moves between devices by JAX's collectives and lax.ppermute only.
A program may use at most 128 MiB of HBM per device.

```python
import jax
import jax.numpy as jnp
from jax import lax

EXPERTS = 64
D_MODEL = 2048
D_EXPERT = 1024


def strengthened(values, key, source, target, parts, factor):
    def block_of(position):
        return (jnp.arange(values.shape[position]) // (values.shape[position] // parts)).reshape((-1,) + (1,) * (values.ndim - 1 - position))

    one_side = jax.random.permutation(key, parts)[block_of(target)]
    far = (block_of(target) + parts // 2) % parts
    return jnp.where((block_of(source) == one_side) | (block_of(source) == far), factor * values, values)


def block_levels(key, extent, shards, least, largest):
    gain, own = 1.0, jax.random.fold_in(key, 6)
    for dim, parts in shards:
        steps = jnp.exp(jax.random.uniform(jax.random.fold_in(own, dim), (parts,), jnp.float32, least / len(shards), largest / len(shards)))
        gain = gain * jnp.repeat(steps, extent[dim] // parts).reshape([-1 if axis == dim else 1 for axis in range(len(extent))])
    return gain


def scatter_about(own_key, dims, spread, limit, cuts=(), dtype=jnp.bfloat16):
    array = jax.random.normal(own_key, dims, jnp.float32) * spread
    if len(cuts) > 0:
        array = block_levels(own_key, dims, cuts, -0.22, 0.18) * array
    return jnp.clip(array, min=-limit, max=limit).astype(dtype)


def gaussian_with(rng, dims, width, bound, cuts, heavy, kind=jnp.bfloat16):
    array = width * jax.random.normal(rng, dims, jnp.float32)
    if cuts:
        array = array * block_levels(rng, dims, cuts, -0.22, 0.18)
    return jnp.clip(strengthened(array, jax.random.fold_in(rng, 3), *heavy), -bound, bound).astype(kind)


def setup_inputs(seed: int = 0) -> dict:
    key_of = jax.random.split(jax.random.key(seed), 5)
    return {
        "w_down": gaussian_with(key_of[0], (EXPERTS, D_EXPERT, D_MODEL), D_EXPERT ** -0.5, 0.25, ((0, 16), (2, 16)), (2, 1, 16, 2.0), jnp.float32),
        "avg_down": scatter_about(key_of[1], (EXPERTS, D_EXPERT, D_MODEL), (D_EXPERT * 4) ** -0.5, 0.09375, ((0, 16), (2, 16))),
        "router_weight": scatter_about(key_of[2], (D_MODEL, EXPERTS), D_MODEL ** -0.5, 0.125, ((0, 16), (1, 16)), jnp.float32),
        "router_gain": jnp.clip(1.0 + 0.15 * jax.random.normal(key_of[3], (D_MODEL,), jnp.float32), 0.25, 1.75),
    }


def reference(w_down, avg_down, router_weight, router_gain):
    fresh_down = w_down + avg_down.astype(jnp.float32)
    scale_down = jnp.sqrt(lax.optimization_barrier(jnp.sum(fresh_down * fresh_down, axis=2)))
    serve_down = (fresh_down / jnp.expand_dims(scale_down, 2)).astype(jnp.bfloat16)
    serve_router = (router_weight * router_gain[:, None]).astype(jnp.bfloat16)
    return (serve_down, scale_down, serve_router)
```

```python
import functools

import jax
import jax.numpy as jnp
from jax import lax
from jax.experimental import pallas as pl
from jax.experimental.pallas import tpu as pltpu
from jax.sharding import PartitionSpec as P


CORES = 2
LANES = 128
MiB = 2**20


def place_kernel(half, chips, plan, *refs):
    blocks, out_ref, sems = refs[: len(plan)], refs[-2], refs[-1]
    me = lax.axis_index("zero")
    core, chip = me % CORES, me // CORES
    sign = 1 - CORES * core
    copies = []
    for block, (step, e, across) in zip(blocks, plan):
        owner = core if not across else 1 - core
        source = (chip + (sign if across else -sign) * step + chips) % chips
        for side in range(CORES):
            column = pl.multiple_of((source * CORES + side) * LANES, LANES)
            here = block.at[side] if e is not None else None
            for n in ([e] if e is not None else range(half)):
                copies.append(
                    pltpu.make_async_copy(
                        here if e is not None else block.at[n, side],
                        out_ref.at[owner * half + n, :, pl.ds(column, LANES)],
                        sems.at[len(copies)],
                    )
                )
    for copy in copies:
        copy.start()
    for copy in copies:
        copy.wait()


def place(out, shape, half, chips, blocks):
    arrays = [b[0] for b in blocks]
    plan = tuple(b[1:] for b in blocks)
    count = sum(CORES * (1 if b[2] is not None else half) for b in blocks)
    any_spec = pl.BlockSpec(memory_space=pl.ANY)
    vmem = pl.BlockSpec(memory_space=pltpu.VMEM)
    size = sum(a.size * 2 for a in arrays)
    return pl.pallas_call(
        functools.partial(place_kernel, half, chips, plan),
        out_shape=jax.ShapeDtypeStruct(shape, jnp.bfloat16),
        in_specs=[vmem] * len(arrays) + ([] if out is None else [any_spec]),
        out_specs=any_spec,
        scratch_shapes=[pltpu.SemaphoreType.DMA((count,))],
        input_output_aliases={} if out is None else {len(arrays): 0},
        compiler_params=pltpu.CompilerParams(vmem_limit_bytes=size + MiB),
        cost_estimate=pl.CostEstimate(flops=0, bytes_accessed=2 * size, transcendentals=0),
    )(*arrays, *([] if out is None else [out]))


def shards(w_down, avg_down, router_weight, router_gain):
  experts, rows, cols = w_down.shape
  half = experts // CORES
  zero = lax.axis_size("zero")
  chips = zero // CORES
  me = lax.axis_index("zero")
  core = me % CORES
  partner = [(i, i ^ 1) for i in range(zero)]
  ring = [(i, (i + (CORES if i % CORES == 0 else -CORES)) % zero) for i in range(zero)]

  def fresh_of(first):
      w = lax.dynamic_slice_in_dim(w_down, first, half, 0)
      a = lax.dynamic_slice_in_dim(avg_down, first, half, 0)
      return w + a.astype(jnp.float32)

  theirs = fresh_of(half * (1 - core))
  other = lax.ppermute(theirs, "zero", partner)
  mine = fresh_of(half * core)

  fresh = w_down + avg_down.astype(jnp.float32)
  sums = jnp.sum(fresh * fresh, axis=2)
  lines = half * rows // 128
  sums = jnp.broadcast_to(sums.reshape(1, CORES, lines, 128), (chips, CORES, lines, 128)).reshape(zero, lines, 128)
  part = (router_weight * router_gain[:, None]).astype(jnp.bfloat16).astype(jnp.float32).T
  part = jnp.broadcast_to(part[None], (zero, *part.shape))
  met = lax.all_to_all(jnp.concatenate([sums, part], axis=1), "zero", split_axis=0, concat_axis=0, tiled=True)
  total = met[:, :lines].sum(axis=0).reshape(half, rows)
  scale = jnp.sqrt(total)
  columns = jnp.moveaxis(met[:, lines:], 0, 1).reshape(part.shape[1], -1).astype(jnp.bfloat16)

  own = (lax.broadcasted_iota(jnp.int32, (CORES, 1, 1), 0) == core)

  def chunk_of(e):
      fresh = jnp.where(own, mine[e][None], other[e][None])
      return (fresh / scale[e][None, :, None]).astype(jnp.bfloat16)

  shape = (experts, rows, cols * zero)
  put = functools.partial(place, shape=shape, half=half, chips=chips)
  out = None
  pending = []
  held = [chunk_of(e) for e in range(half)]
  for step in range(chips):
      following = []
      for e in range(half):
          if step < chips - 1:
              following.append(lax.ppermute(held[e], "zero", ring))
          blocks = [(held[e], step, e, False)]
          if step < chips - 1:
              if e == half - 1:
                  both = jnp.stack(held)
                  pending.append((lax.ppermute(both, "zero", partner), step, None, True))
              elif pending:
                  blocks.append(pending.pop())
          else:
              got = (lax.ppermute(held[e], "zero", partner), step, e, True)
              if pending:
                  blocks.append(pending.pop())
              pending.append(got)
          out = put(out, blocks=blocks)
      held = following
  out = put(out, blocks=pending)

  scale_other = lax.ppermute(scale, "zero", partner)
  scale_down = jnp.where(core == 0, jnp.concatenate([scale, scale_other]), jnp.concatenate([scale_other, scale]))

  bank = lax.axis_index("bank")
  n = lax.axis_size("bank")
  side = 4 if n == 16 else 1
  x, y = bank % side, bank // side

  def along(block, index, shift_of):
      gathered = jnp.zeros((side, *block.shape), block.dtype)
      gathered = lax.dynamic_update_slice_in_dim(gathered, block[None], index, 0)
      for k in range(1, side):
          got = lax.ppermute(block, "bank", [(b, shift_of(b, k)) for b in range(n)])
          gathered = lax.dynamic_update_slice_in_dim(gathered, got[None], (index - k) % side, 0)
      return gathered.reshape(side * block.shape[0], *block.shape[1:])

  columns = along(columns, x, lambda b, k: b // side * side + (b % side + k) % side)
  columns = along(columns, y, lambda b, k: (b + k * side) % n)
  return out, scale_down, columns.T


def solution(mesh):
    return jax.shard_map(
        shards,
        mesh=mesh,
        in_specs=(P("bank", None, "zero"), P("bank", None, "zero"), P("zero", "bank"), P("zero")),
        out_specs=(P("bank", None, None), P("bank", None), P()),
        check_vma=False,
    )
```
